32 devices in a mesh: gx: 2 (over x), gy: 4 (over y, core), gz: 4 (over z).
Axes of the slice: x: 2, y: 2, z: 4, core: 2. Of those that a mesh axis runs over, the one named last changes fastest.
Arguments:
- density: float32 [10, 20, 640], P('gx', 'gy', 'gz'), may hold values from 0.5 to 2
- velocity: float32 [3, 10, 20, 640], P(None, 'gx', 'gy', 'gz'), may hold values from -3.2 to 3.2
- pressure: float32 [10, 20, 640], P('gx', 'gy', 'gz'), may hold values from 0.5 to 2
- blending: float32 [2, 4, 128], P('gx', 'gy', 'gz'), may hold values from 0 to 0.6
- face_signal_weights: bfloat16 [4, 1280, 4096], P(None, ('gx', 'gy'), 'gz'), may hold values from -0.03125 to 0.03125
- surf_id: int32 [3840], P(('gx', 'gy', 'gz')), may hold values from -1 to 1279, as said below
- surface_face_code: int32 [3840], P(('gx', 'gy', 'gz')), may hold values from 0 to 191, as said below
Outputs:
- tendency: float32 [5, 10, 20, 640], P(None, 'gx', 'gy', 'gz')
- signals: float32 [4096], P(('gz', 'gx', 'gy'))
The draws below stay inside these ranges and needn't reach their ends.
Inputs may be any that keep to these rules, and one draw needn't show every extreme that they name: `surf_id`: every face id 0 to 1279 stands in exactly one slot; a device's listed faces fill its first slots and its other slots hold -1. A quarter of the devices list exactly 120 faces, the others at most 40. `surface_face_code`: the codes of one device are distinct.
All inputs are finite; a program needn't handle non-finite values.
Results may differ from the reference program's by a relative error of at most 0.0029.
Values may be sent and summed in bfloat16 or wider, within the bound.
A program may use at most 128 MiB of HBM per device.

```python
import math
import jax
import jax.numpy as jnp
import numpy as np
from jax import lax

QN = 4
EX = 1
EY = 1
EZ = 32
FACE_DEV = 40
ALL_DEVICES = 32
ELEMS = 32
SLOTS = 120
FACES = 1280
SIG = 4096
ELEMENTS_FIRST = 2
ELEMENTS_SECOND = 4
ELEMENTS_THIRD = 128
NX = 10
NY = 20
NZ = 640
N_GX = 2
N_GY = 4
N_GZ = 4


def face_counts(key):
    group_total = ALL_DEVICES // 4
    device_order = jax.random.permutation(jax.random.fold_in(key, 1), ALL_DEVICES).astype(jnp.int32)
    second = jax.random.randint(jax.random.fold_in(key, 2), (group_total,), 0, FACE_DEV + 1, dtype=jnp.int32)
    third = jax.random.randint(jax.random.fold_in(key, 3), (group_total,), 0, FACE_DEV + 1, dtype=jnp.int32) % (FACE_DEV - second + 1)
    fourth = FACE_DEV - second - third
    busiest = jnp.full((group_total,), SLOTS, dtype=jnp.int32)
    in_order = jnp.stack([busiest, second, third, fourth], axis=1).reshape(-1)
    return jnp.zeros((ALL_DEVICES,), jnp.int32).at[device_order].set(in_order)


def draw_surf_id(key, part):
    counts = face_counts(jax.random.fold_in(key, 101))
    offsets = jnp.cumsum(counts) - counts
    shuffled = jax.random.permutation(jax.random.fold_in(key, 102), FACES).astype(jnp.int32)
    slot_index = jnp.arange(SLOTS, dtype=jnp.int32)
    occupied = slot_index[None, :] < counts[:, None]
    position = jnp.clip(offsets[:, None] + slot_index[None, :], 0, FACES - 1)
    return jnp.where(occupied, shuffled[position], -1).reshape(-1).astype(jnp.int32)


def draw_surface_face_code(key, part):
    device_keys = jax.random.split(jax.random.fold_in(key, 201), ALL_DEVICES)

    def one_device(device_key):
        return jax.random.permutation(device_key, 6 * ELEMS)[:SLOTS]
    return jax.vmap(one_device)(device_keys).reshape(-1).astype(jnp.int32)


def raised(entries, stream_key, source, target, shards_of, factor):
    def block_of(axis_at):
        return (jnp.arange(entries.shape[axis_at]) // (entries.shape[axis_at] // shards_of)).reshape((-1,) + (1,) * (entries.ndim - 1 - axis_at))

    one_side = jax.random.permutation(stream_key, shards_of)[block_of(target)]
    second = (block_of(target) + shards_of // 2) % shards_of
    return jnp.where((block_of(source) == one_side) | (block_of(source) == second), factor * entries, entries)


def block_scale(stream_key, extent, cuts, smallest, largest):
    def one(dim, parts):
        steps = jax.random.uniform(jax.random.fold_in(jax.random.fold_in(stream_key, 6), dim), (parts,), jnp.float32, smallest / len(cuts), largest / len(cuts))
        return jnp.repeat(jnp.exp(steps), extent[dim] // parts).reshape((-1,) + (1,) * (len(extent) - dim - 1))

    level = one(*cuts[0])
    for cut in cuts[1:]:
        level = level * one(*cut)
    return level


def noise(own_key, extent, scale, bound, pieces=(), held_as=jnp.bfloat16):
    entries = jax.random.normal(own_key, extent, jnp.float32) * scale
    if len(pieces) > 0:
        entries = block_scale(own_key, extent, pieces, -0.22, 0.18) * entries
    return jnp.clip(entries, min=-bound, max=bound).astype(held_as)


def noise_with(stream_key, shape, width, limit, shards, heavy, kind=jnp.bfloat16):
    values = width * jax.random.normal(stream_key, shape, jnp.float32)
    if shards:
        values = values * block_scale(stream_key, shape, shards, -0.22, 0.18)
    return jnp.clip(raised(values, jax.random.fold_in(stream_key, 3), *heavy), -limit, limit).astype(kind)


def setup_inputs(seed: int = 0) -> dict:
    key_of = jax.random.split(jax.random.key(seed), 8)
    return {
        "density": jnp.clip(jnp.exp(math.log(2.0) - 1.3862944 * jax.random.uniform(key_of[0], (NX, NY, NZ), jnp.float32) ** block_scale(key_of[0], (NX, NY, NZ), ((0, 2), (1, 4), (2, 4)), -0.2, 0.2)), 0.5, 2.0),
        "velocity": noise(key_of[1], (3, NX, NY, NZ), 0.8, 3.2, ((1, 2), (2, 4), (3, 4)), jnp.float32),
        "pressure": jnp.clip(jnp.exp(math.log(2.0) - 1.3862944 * jax.random.uniform(key_of[2], (NX, NY, NZ), jnp.float32) ** block_scale(key_of[2], (NX, NY, NZ), ((0, 2), (1, 4), (2, 4)), -0.2, 0.2)), 0.5, 2.0),
        "blending": jnp.clip(0.6 * jax.random.uniform(key_of[3], (ELEMENTS_FIRST, ELEMENTS_SECOND, ELEMENTS_THIRD), jnp.float32) ** block_scale(key_of[3], (ELEMENTS_FIRST, ELEMENTS_SECOND, ELEMENTS_THIRD), ((0, 2), (1, 4), (2, 4)), -0.2, 0.2), 0.0, 0.6),
        "face_signal_weights": noise_with(key_of[4], (QN, FACES, SIG), (16 * QN * FACES) ** -0.5, 0.03125, ((1, 8), (2, 4)), (1, 2, 8, 2.0)),
        "surf_id": draw_surf_id(jax.random.fold_in(key_of[7], 71), 0),
        "surface_face_code": draw_surface_face_code(jax.random.fold_in(key_of[7], 71), 0),
    }


GAMMA = 1.4

def gauss_lobatto():
    inner_root = math.sqrt(3.0 / 7.0)
    points = np.array([-1.0, -inner_root, 0.0, inner_root, 1.0])
    quad_weights = np.array([0.1, 49.0 / 90.0, 32.0 / 45.0, 49.0 / 90.0, 0.1])
    barycentric = np.ones(5)
    for target in range(5):
        for source in range(5):
            if source != target:
                barycentric[target] = barycentric[target] / (points[target] - points[source])
    derivative = np.zeros((5, 5))
    for target in range(5):
        for source in range(5):
            if source != target:
                derivative[target, source] = barycentric[source] / barycentric[target] / (points[target] - points[source])
        derivative[target, target] = -np.sum(derivative[target])
    return (derivative, quad_weights)

def energy_of(prim):
    speed_square = prim[1] * prim[1] + prim[2] * prim[2] + prim[3] * prim[3]
    return prim[4] / (GAMMA - 1.0) + 0.5 * prim[0] * speed_square

def conserved(prim):
    return jnp.stack([prim[0], prim[0] * prim[1], prim[0] * prim[2], prim[0] * prim[3], energy_of(prim)])

def physical_flux(prim, normal):
    mass_flux = prim[0] * prim[normal]
    flux_parts = [mass_flux]
    for field_component in (1, 2, 3):
        momentum = mass_flux * prim[field_component]
        if field_component == normal:
            momentum = momentum + prim[4]
        flux_parts.append(momentum)
    flux_parts.append((energy_of(prim) + prim[4]) * prim[normal])
    return jnp.stack(flux_parts)

def wave_speed(prim, normal):
    return jnp.abs(prim[normal]) + jnp.sqrt(GAMMA * prim[4] / prim[0])

def rusanov(left, right, normal):
    fastest = jnp.maximum(wave_speed(left, normal), wave_speed(right, normal))
    return 0.5 * (physical_flux(left, normal) + physical_flux(right, normal)) - 0.5 * fastest * (conserved(right) - conserved(left))

def split_flux(left, right, normal):
    density = 0.5 * (left[0] + right[0])
    pressure = 0.5 * (left[4] + right[4])
    mean_normal = 0.5 * (left[normal] + right[normal])
    specific = 0.5 * (energy_of(left) / left[0] + energy_of(right) / right[0])
    mass_flux = density * mean_normal
    flux_parts = [mass_flux]
    for field_component in (1, 2, 3):
        momentum = mass_flux * (0.5 * (left[field_component] + right[field_component]))
        if field_component == normal:
            momentum = momentum + pressure
        flux_parts.append(momentum)
    flux_parts.append(mass_flux * specific + pressure * mean_normal)
    return jnp.stack(flux_parts)

def direction_terms(core, lower, upper, node_factors, axis_dim):
    derivative, quad_weights = gauss_lobatto()
    node_count = derivative.shape[0]
    full_shape = core.shape
    elem_count = full_shape[axis_dim] // node_count
    split_shape = full_shape[:axis_dim] + (elem_count, node_count) + full_shape[axis_dim + 1:]
    ghost_shape = full_shape[:axis_dim] + (1, 1) + full_shape[axis_dim + 1:]
    node_axis = axis_dim + 1
    node_shape = [1] * len(split_shape)
    node_shape[node_axis] = node_count
    node_shape = tuple(node_shape)
    by_element = core.reshape(split_shape)
    blend_split = node_factors.reshape(split_shape[1:])[None]
    high_order = jnp.zeros(split_shape, jnp.float32)
    for column in range(node_count):
        partner = lax.slice_in_dim(by_element, column, column + 1, axis=node_axis)
        factor = jnp.asarray(2.0 * derivative[:, column], jnp.float32).reshape(node_shape)
        high_order = high_order + factor * split_flux(by_element, partner, axis_dim)
    node_flux = physical_flux(by_element, axis_dim)
    inner_flux = rusanov(lax.slice_in_dim(by_element, 0, node_count - 1, axis=node_axis), lax.slice_in_dim(by_element, 1, node_count, axis=node_axis), axis_dim)
    edge_flux = jnp.concatenate([lax.slice_in_dim(node_flux, 0, 1, axis=node_axis), inner_flux, lax.slice_in_dim(node_flux, node_count - 1, node_count, axis=node_axis)], axis=node_axis)
    weight_row = jnp.asarray(quad_weights, jnp.float32).reshape(node_shape)
    low_order = (lax.slice_in_dim(edge_flux, 1, node_count + 1, axis=node_axis) - lax.slice_in_dim(edge_flux, 0, node_count, axis=node_axis)) / weight_row
    volume = high_order + blend_split * (low_order - high_order)
    first_nodes = lax.slice_in_dim(by_element, 0, 1, axis=node_axis)
    last_nodes = lax.slice_in_dim(by_element, node_count - 1, node_count, axis=node_axis)
    left_states = jnp.concatenate([lower.reshape(ghost_shape), last_nodes], axis=axis_dim)
    right_states = jnp.concatenate([first_nodes, upper.reshape(ghost_shape)], axis=axis_dim)
    face_flux = rusanov(left_states, right_states, axis_dim)
    lower_term = -(lax.slice_in_dim(face_flux, 0, elem_count, axis=axis_dim) - lax.slice_in_dim(node_flux, 0, 1, axis=node_axis)) / float(quad_weights[0])
    upper_term = (lax.slice_in_dim(face_flux, 1, elem_count + 1, axis=axis_dim) - lax.slice_in_dim(node_flux, node_count - 1, node_count, axis=node_axis)) / float(quad_weights[-1])
    middle_shape = list(split_shape)
    middle_shape[node_axis] = node_count - 2
    surface = jnp.concatenate([lower_term, jnp.zeros(tuple(middle_shape), jnp.float32), upper_term], axis=node_axis)
    return (volume + surface).reshape(full_shape)

def tendency_of(core, ghosts, node_factors):
    running = jnp.zeros(core.shape, jnp.float32)
    for axis_dim in (1, 2, 3):
        running = running - direction_terms(core, ghosts[axis_dim - 1][0], ghosts[axis_dim - 1][1], node_factors, axis_dim)
    return running

def node_blend(blend_factors, node_count):
    first_count, second_count, third_count = blend_factors.shape
    widened = jnp.broadcast_to(blend_factors[:, None, :, None, :, None], (first_count, node_count, second_count, node_count, third_count, node_count))
    return widened.reshape(first_count * node_count, second_count * node_count, third_count * node_count)

def face_sources(values, face_code, elem_total):
    face_index = face_code // elem_total
    normal_dim = face_index // 2
    sign = (2 * (face_index % 2) - 1).astype(jnp.float32)
    picks = (normal_dim[:, None] == jnp.arange(3, dtype=jnp.int32)[None, :]).astype(jnp.float32)
    normal_speed = sign[:, None] * (picks[:, 0:1] * values[1] + picks[:, 1:2] * values[2] + picks[:, 2:3] * values[3])
    quad_weights = gauss_lobatto()[1]
    surface_weights = jnp.asarray(np.outer(quad_weights, quad_weights).reshape(-1), jnp.float32)
    mass_flux = values[0] * normal_speed
    quantities = [mass_flux]
    for field_component in (1, 2, 3):
        quantities.append(values[4] * (sign[:, None] * picks[:, field_component - 1:field_component]) + mass_flux * values[field_component])
    return jnp.stack([lax.optimization_barrier(jnp.sum(surface_weights * amount, axis=1)) for amount in quantities])

def reference(density, velocity, pressure, blending, face_signal_weights, surf_id, surface_face_code):
    primitive = jnp.concatenate([density[None], velocity, pressure[None]], axis=0)
    node_count = 5
    wrapped_around = jnp.concatenate([primitive[:, -1:], primitive, primitive[:, :1]], axis=1)

    def slab_terms(slab_index):
        window = lax.dynamic_slice_in_dim(wrapped_around, slab_index * node_count, node_count + 2, 1)
        slab_core = window[:, 1:-1]
        ghosts = ((window[:, 0:1], window[:, -1:]), (slab_core[:, :, -1:], slab_core[:, :, :1]), (slab_core[:, :, :, -1:], slab_core[:, :, :, :1]))
        node_factors = node_blend(lax.dynamic_slice_in_dim(blending, slab_index, 1, 0), node_count)
        return tendency_of(slab_core, ghosts, node_factors)
    slab_all = lax.map(slab_terms, jnp.arange(ELEMENTS_FIRST, dtype=jnp.int32))
    tendency = jnp.transpose(slab_all, (1, 0, 2, 3, 4)).reshape(primitive.shape)
    slot_total = surface_face_code.shape[0]
    slot_index = jnp.arange(slot_total, dtype=jnp.int32)
    device = slot_index // SLOTS
    owner_x = device // (N_GY * N_GZ)
    owner_y = device // N_GZ % N_GY
    owner_z = device % N_GZ
    elem_total = EX * EY * EZ
    face_index = surface_face_code // elem_total
    mesh_element = surface_face_code % elem_total
    elem_x = owner_x * EX + mesh_element // (EY * EZ)
    elem_y = owner_y * EY + mesh_element // EZ % EY
    elem_z = owner_z * EZ + mesh_element % EZ
    normal_dim = (face_index // 2)[:, None, None]
    fixed_node = (face_index % 2 * (node_count - 1))[:, None, None]
    across_first = jnp.arange(node_count, dtype=jnp.int32)[None, :, None]
    across_second = jnp.arange(node_count, dtype=jnp.int32)[None, None, :]
    base_x = (elem_x * node_count)[:, None, None]
    base_y = (elem_y * node_count)[:, None, None]
    base_z = (elem_z * node_count)[:, None, None]
    index_x = jnp.where(normal_dim == 0, base_x + fixed_node, base_x + across_first)
    index_y = jnp.where(normal_dim == 0, base_y + across_first, jnp.where(normal_dim == 1, base_y + fixed_node, base_y + across_second))
    index_z = jnp.where(normal_dim == 2, base_z + fixed_node, base_z + across_second)
    values = primitive[:, index_x, index_y, index_z].reshape(5, slot_total, node_count * node_count)
    face_data = face_sources(values, surface_face_code, elem_total).astype(jnp.bfloat16)
    placed = jnp.where(surf_id >= 0, surf_id, FACES).astype(jnp.int32)
    surface_data = jnp.zeros((QN, FACES), jnp.bfloat16).at[:, placed].set(face_data, mode='drop')
    group_faces = FACES // (N_GX * N_GY)

    def add_group(group_index, running):
        first_face = (group_index * group_faces).astype(jnp.int32)
        data_block = lax.dynamic_slice_in_dim(surface_data, first_face, group_faces, 1).reshape(-1)
        weight_block = lax.dynamic_slice_in_dim(face_signal_weights, first_face, group_faces, 1).reshape(QN * group_faces, SIG)
        return running + jnp.dot(data_block, weight_block, preferred_element_type=jnp.float32)
    signals = lax.fori_loop(0, N_GX * N_GY, add_group, jnp.zeros((SIG,), jnp.float32))
    return (tendency, signals)
```

```python
import functools
import math

import jax
import jax.numpy as jnp
import numpy as np
from jax import lax
from jax.experimental import pallas as pl
from jax.experimental.pallas import tpu as pltpu
from jax.sharding import PartitionSpec as P

GAMMA = 1.4
MESH = pl.DeviceIdType.MESH
F32 = jnp.float32
BF16 = jnp.bfloat16


def gauss_lobatto():
    inner_root = math.sqrt(3.0 / 7.0)
    points = np.array([-1.0, -inner_root, 0.0, inner_root, 1.0])
    quad_weights = np.array([0.1, 49.0 / 90.0, 32.0 / 45.0, 49.0 / 90.0, 0.1])
    barycentric = np.ones(5)
    for target in range(5):
        for source in range(5):
            if source != target:
                barycentric[target] = barycentric[target] / (points[target] - points[source])
    derivative = np.zeros((5, 5))
    for target in range(5):
        for source in range(5):
            if source != target:
                derivative[target, source] = (
                    barycentric[source] / barycentric[target] / (points[target] - points[source])
                )
        derivative[target, target] = -np.sum(derivative[target])
    return (derivative, quad_weights)


DERIV, QUAD = gauss_lobatto()
NODES = len(QUAD)


def up(value, step):
    return (value + step - 1) // step * step


def pick(index, table):
    out = jnp.zeros(index.shape, F32)
    for key, value in table.items():
        out = jnp.where(index == key, F32(value), out)
    return out


def with_energy(prim):
    rho, u, v, w, p = prim
    specific = p / rho * (1.0 / (GAMMA - 1.0)) + 0.5 * (u * u + v * v + w * w)
    return (rho, u, v, w, specific, p)


def pair_flux(a, b, d):
    r, s1, s2, s3, se, sp = (x + y for x, y in zip(a, b))
    speeds = (s1, s2, s3)
    m = r * speeds[d]
    parts = [m + m]
    for c in range(3):
        parts.append(m * speeds[c] + 4.0 * sp if c == d else m * speeds[c])
    parts.append(m * se + 2.0 * (sp * speeds[d]))
    return parts


def node_state(a, d):
    rho, u, v, w, specific, p = a
    speeds = (u, v, w)
    energy = rho * specific
    cons = [rho, rho * u, rho * v, rho * w, energy]
    normal = speeds[d]
    flux = [cons[1 + d]]
    for c in range(3):
        part = cons[1 + c] * normal
        flux.append(part + p if c == d else part)
    flux.append((energy + p) * normal)
    return flux, cons, jnp.abs(normal) + jnp.sqrt(GAMMA * (p / rho))


def rusanov2(left, right):
    (fl, ul, sl), (fr, ur, sr) = left, right
    fastest = jnp.maximum(sl, sr)
    return [a + b - fastest * (d - c) for a, b, c, d in zip(fl, fr, ul, ur)]


def kernel(
    sizes,
    den_h, vel_h, pre_h, ble_h, wei_h, id_h, code_h,
    tend_ref, sig_ref,
    den, vel, pre, ble, wei, ids, codes,
    prim, acc, coef, ystage, yghost, zstage, zghost,
    mine, faces_in, part, parts_in, stage, sums_in,
    in_sem, halo_send, halo_recv, face_send, face_recv, z_send, z_recv, rs_send, rs_recv,
):
    nx_dev, ny_dev, nz_dev = sizes
    groups = nx_dev * ny_dev
    px, py, pz = den_h.shape
    elems = ble_h.shape[-1]
    slots = id_h.shape[-1]
    lanes = prim.shape[-1]
    rows = prim.shape[-2]
    quantities, shard_faces, local_signals = wei_h.shape
    own = local_signals // groups

    gx, gy, gz = lax.axis_index("gx"), lax.axis_index("gy"), lax.axis_index("gz")
    group = gx * ny_dev + gy

    def in_group(step):
        other = lax.rem(group + step, groups)
        return (lax.div(other, ny_dev), lax.rem(other, ny_dev), gz)

    def in_column(step):
        return (gx, gy, lax.rem(gz + step, nz_dev))

    barrier = pltpu.get_barrier_semaphore()
    for step in range(1, groups):
        pl.semaphore_signal(barrier, inc=1, device_id=in_group(step), device_id_type=MESH)
    for step in range(1, nz_dev):
        pl.semaphore_signal(barrier, inc=1, device_id=in_column(step), device_id_type=MESH)

    loads = [
        pltpu.make_async_copy(src, dst, in_sem.at[n])
        for n, (src, dst) in enumerate(
            ((den_h, den), (vel_h, vel), (pre_h, pre), (ble_h, ble), (id_h, ids), (code_h, codes), (wei_h, wei))
        )
    ]
    for load in loads:
        load.start()

    row = lax.broadcasted_iota(jnp.int32, (rows, lanes), 0)
    lane = lax.broadcasted_iota(jnp.int32, (rows, lanes), 1)
    lane_node = lax.rem(lane, NODES)
    row_weight = pick(row, {i: QUAD[i] for i in range(NODES)})

    width = up(3 * elems, 128)
    z_at = lax.broadcasted_iota(jnp.int32, (lanes, width), 0)
    c_at = lax.broadcasted_iota(jnp.int32, (lanes, width), 1)
    element = lax.div(z_at, NODES)
    node = z_at - NODES * element
    reduce_z = jnp.where(element == c_at, pick(node, {i: QUAD[i] for i in range(NODES)}), F32(0))
    reduce_z = jnp.where((element + elems == c_at) & (node == 0), F32(-1), reduce_z)
    reduce_z = jnp.where((element + 2 * elems == c_at) & (node == NODES - 1), F32(1), reduce_z)
    reduce_z = jnp.where(z_at < pz, reduce_z, F32(0))

    prim[:, 0:px] = jnp.ones((5, px, rows, lanes), F32)
    for n in range(3):
        loads[n].wait()
    for x in range(px):
        prim[0, x, 0:py, 0:pz] = den[x]
        for c in range(3):
            prim[1 + c, x, 0:py, 0:pz] = vel[c, x]
        prim[4, x, 0:py, 0:pz] = pre[x]

    def mass_momentum(x, d):
        rho, u, v, w, p = (prim[f, x] for f in range(5))
        speeds = (u, v, w)
        m = rho * speeds[d]
        return [m] + [m * speeds[c] + p if c == d else m * speeds[c] for c in range(3)]

    def rows_of(values, sign):
        out = jnp.zeros((rows, lanes), F32)
        for q in range(quantities):
            out = jnp.where(row == q, sign * values[q], out)
        return out

    tables = []
    for x, sign in ((0, -1.0), (px - 1, 1.0)):
        sums = [jnp.sum(row_weight * f, axis=0, keepdims=True) for f in mass_momentum(x, 0)]
        tables.append(rows_of(sums, sign))
    along_y = [jnp.zeros((rows, lanes), F32)] * quantities
    along_z = [jnp.zeros((rows, lanes), F32)] * quantities
    for x in range(px):
        along_y = [a + F32(QUAD[x]) * f for a, f in zip(along_y, mass_momentum(x, 1))]
        along_z = [a + F32(QUAD[x]) * f for a, f in zip(along_z, mass_momentum(x, 2))]
    for y, sign in ((0, -1.0), (py - 1, 1.0)):
        tables.append(rows_of([a[y : y + 1] for a in along_y], sign))
    tables.append(rows_of([jnp.sum(row_weight * a, axis=0, keepdims=True) for a in along_z], 1.0))
    table = jnp.dot(
        jnp.concatenate(tables, axis=0), reduce_z,
        precision=lax.Precision.HIGHEST, preferred_element_type=F32,
    ).astype(BF16)

    for n in range(3, 6):
        loads[n].wait()
    pad = mine.shape[-1]
    code_row = jnp.concatenate([codes[...], jnp.full((1, pad - slots), -1, jnp.int32)], axis=1) if pad > slots else codes[...]
    id_row = jnp.concatenate([ids[...], jnp.full((1, pad - slots), -1, jnp.int32)], axis=1) if pad > slots else ids[...]
    r_at = lax.broadcasted_iota(jnp.int32, (width, pad), 0)
    chosen = []
    for f in range(4):
        hit = (code_row == r_at + f * elems) & (r_at < elems)
        chosen.append(jnp.where(hit, F32(1), F32(0)).astype(BF16))
    hit = (code_row == r_at + 3 * elems) & (r_at >= elems) & (r_at < 3 * elems)
    chosen.append(jnp.where(hit, F32(1), F32(0)).astype(BF16))
    face_values = jnp.dot(
        jnp.concatenate([table[rows * f : rows * f + rows] for f in range(5)], axis=1),
        jnp.concatenate(chosen, axis=0),
        preferred_element_type=F32,
    )
    slot_row = lax.broadcasted_iota(jnp.int32, (rows, pad), 0)
    mine[...] = jnp.where(slot_row == quantities, id_row.astype(F32), face_values)

    ystage[...] = jnp.ones(ystage.shape, F32)
    for x in range(px):
        for f in range(5):
            ystage[0, f, x : x + 1, :] = prim[f, x, 0:1, :]
            ystage[1, f, x : x + 1, :] = prim[f, x, py - 1 : py, :]
    zlane = lax.broadcasted_iota(jnp.int32, (rows, 128), 1)
    for side, at in ((0, 0), (1, pz - 1)):
        packed = jnp.ones((rows, 128), F32)
        for f in range(5):
            for x in range(px):
                packed = jnp.where(zlane == f * px + x, prim[f, x, :, at : at + 1], packed)
        zstage[side] = packed

    pl.semaphore_wait(barrier, groups - 1 + nz_dev - 1)

    def remote(src, dst, send, recv, device):
        return pltpu.make_async_remote_copy(
            src_ref=src, dst_ref=dst, send_sem=send, recv_sem=recv, device_id=device, device_id_type=MESH
        )

    face_copies = [
        remote(mine, faces_in.at[k - 1], face_send.at[k - 1], face_recv.at[k - 1], in_group(k))
        for k in range(1, groups)
    ]
    for copy in face_copies:
        copy.start()

    def beside(axis, step):
        at = [gx, gy, gz]
        at[axis] = lax.rem(at[axis] + sizes[axis] + step, sizes[axis])
        return tuple(at)

    halo_copies = [
        remote(prim.at[:, px - 1], prim.at[:, px + 1], halo_send.at[0], halo_recv.at[0], beside(0, 1)),
        remote(prim.at[:, 0], prim.at[:, px], halo_send.at[1], halo_recv.at[1], beside(0, -1)),
        remote(ystage.at[1], yghost.at[0], halo_send.at[2], halo_recv.at[2], beside(1, 1)),
        remote(ystage.at[0], yghost.at[1], halo_send.at[3], halo_recv.at[3], beside(1, -1)),
        remote(zstage.at[1], zghost.at[0], halo_send.at[4], halo_recv.at[4], beside(2, 1)),
        remote(zstage.at[0], zghost.at[1], halo_send.at[5], halo_recv.at[5], beside(2, -1)),
    ]
    for copy in halo_copies:
        copy.start()

    spread_e = lax.broadcasted_iota(jnp.int32, (elems, lanes), 0)
    spread_z = lax.broadcasted_iota(jnp.int32, (elems, lanes), 1)
    spread = jnp.where(lax.div(spread_z, NODES) == spread_e, F32(1), F32(0))
    alpha = jnp.dot(
        jnp.broadcast_to(ble[0], (rows, elems)), spread,
        precision=lax.Precision.HIGHEST, preferred_element_type=F32,
    )
    volume = jnp.where(lane < pz, (alpha - 1.0) * 0.25, F32(0))
    for d, at in ((0, row), (1, lane_node)):
        for k in range(1, NODES):
            base = 8 * d + 2 * (k - 1)
            coef[base] = volume * pick(at, {i: DERIV[i, i + k] for i in range(NODES - k)})
            coef[base + 1] = volume * pick(at, {i: DERIV[i + k, i] for i in range(NODES - k)})
        half = pick(at, {i: 0.5 / QUAD[i] for i in range(NODES)})
        coef[16 + 2 * d] = -half * jnp.where(at == NODES - 1, F32(1), alpha)
        coef[17 + 2 * d] = half * jnp.where(at == 0, F32(1), alpha)
    coef[20] = volume
    coef[21] = alpha

    def plane(x):
        return with_energy(tuple(prim[f, x] for f in range(5)))

    def inside(x, carry):
        here = plane(x)
        total = [acc[q, x] for q in range(5)]
        for d, axis, size in ((1, 0, rows), (2, 1, lanes)):
            for k in range(1, NODES):
                there = tuple(pltpu.roll(a, size - k, axis) for a in here)
                flux = pair_flux(here, there, d)
                base = 8 * (d - 1) + 2 * (k - 1)
                forward, back = coef[base], coef[base + 1]
                total = [t + forward * f + pltpu.roll(back * f, k, axis) for t, f in zip(total, flux)]
        for q in range(5):
            acc[q, x] = total[q]
        return carry

    planes = [plane(x) for x in range(px)]
    for x in range(px):
        total = [jnp.zeros((rows, lanes), F32)] * 5
        for other in range(px):
            if other != x:
                flux = pair_flux(planes[x], planes[other], 0)
                total = [t + F32(DERIV[x, other]) * f for t, f in zip(total, flux)]
        for q in range(5):
            acc[q, x] = coef[20] * total[q]
    lax.fori_loop(0, px, inside, 0, unroll=True)

    for copy in face_copies:
        copy.wait()
    wanted = lax.broadcasted_iota(jnp.int32, (shard_faces, pad), 0).astype(F32)
    start = (group * shard_faces).astype(F32)
    arrived = [mine[...]] + [faces_in[k] for k in range(groups - 1)]
    placing = [
        jnp.where(a[quantities : quantities + 1] - start == wanted, F32(1), F32(0)).astype(BF16) for a in arrived
    ]
    part[...] = lax.dot_general(
        jnp.concatenate([a.astype(BF16) for a in arrived], axis=1),
        jnp.concatenate(placing, axis=1),
        (((1,), (1,)), ((), ())),
        preferred_element_type=F32,
    )
    z_copies = [
        remote(part, parts_in.at[k - 1], z_send.at[k - 1], z_recv.at[k - 1], in_column(k))
        for k in range(1, nz_dev)
    ]
    for copy in z_copies:
        copy.start()

    for copy in halo_copies:
        copy.wait()
    low, high = zghost[0], zghost[1]
    for f in range(5):
        for x in range(px):
            prim[f, x, py : py + 1, :] = yghost[1, f, x : x + 1, :]
            prim[f, x, rows - 1 : rows, :] = yghost[0, f, x : x + 1, :]
            at = f * px + x
            first = pz // 128 * 128
            block = prim[f, x, :, first : first + 128]
            block = jnp.where(zlane == pz - first, high[:, at : at + 1], block)
            if first + 128 == lanes:
                block = jnp.where(zlane == 127, low[:, at : at + 1], block)
            else:
                last = prim[f, x, :, lanes - 128 : lanes]
                prim[f, x, :, lanes - 128 : lanes] = jnp.where(zlane == 127, low[:, at : at + 1], last)
            prim[f, x, :, first : first + 128] = block

    def between(x, carry):
        here = plane(x)
        total = [acc[q, x] for q in range(5)]
        for d, axis, size in ((1, 0, rows), (2, 1, lanes)):
            state = node_state(here, d)
            after = (
                [pltpu.roll(a, size - 1, axis) for a in state[0]],
                [pltpu.roll(a, size - 1, axis) for a in state[1]],
                pltpu.roll(state[2], size - 1, axis),
            )
            upper, lower = coef[14 + 2 * d], coef[15 + 2 * d]
            edge = rusanov2(state, after)
            total = [t + upper * e + lower * pltpu.roll(e, 1, axis) for t, e in zip(total, edge)]
        for q in range(5):
            acc[q, x] = total[q]
        return carry

    lax.fori_loop(0, px, between, 0, unroll=True)

    before = node_state(plane(px + 1), 0)
    current = node_state(plane(0), 0)
    below = rusanov2(before, current)
    for x in range(px):
        following = node_state(plane(x + 1), 0)
        above = rusanov2(current, following)
        half = F32(0.5 / QUAD[x])
        for q in range(5):
            out = acc[q, x]
            mix = coef[21] * half
            out = out - (half if x == px - 1 else mix) * above[q]
            out = out + (half if x == 0 else mix) * below[q]
            tend_ref[q, x] = out[0:py, 0:pz]
        current, below = following, above

    for copy in z_copies:
        copy.wait()
    loads[6].wait()
    data = part[...]
    for k in range(nz_dev - 1):
        data = data + parts_in[k]
    data = data.astype(BF16)
    data_row = lax.broadcasted_iota(jnp.int32, data.shape, 0)
    result = jnp.zeros((rows, local_signals), F32)
    for q in range(quantities):
        result = result + jnp.dot(
            jnp.where(data_row == q, data, jnp.zeros((), BF16)), wei[q], preferred_element_type=F32
        )
    result = jnp.sum(result, axis=0, keepdims=True)
    for t in range(groups):
        stage[t] = result[:, t * own : (t + 1) * own]
    rs_copies = []
    for k in range(1, groups):
        other = lax.rem(group + k, groups)
        rs_copies.append(
            remote(stage.at[other], sums_in.at[k - 1], rs_send.at[k - 1], rs_recv.at[k - 1], in_group(k))
        )
    for copy in rs_copies:
        copy.start()
    for copy in rs_copies:
        copy.wait()
    total = stage[group]
    for k in range(groups - 1):
        total = total + sums_in[k]
    sig_ref[...] = total


def shards(sizes, density, velocity, pressure, blending, face_signal_weights, surf_id, surface_face_code):
    groups = sizes[0] * sizes[1]
    px, py, pz = density.shape
    assert blending.shape[:2] == (1, 1) and px == NODES and py == NODES
    rows, lanes = up(py + 2, 8), up(pz + 2, 128)
    slots = surf_id.shape[0]
    pad = up(slots, 128)
    quantities, shard_faces, local_signals = face_signal_weights.shape
    own = local_signals // groups
    dma = pltpu.SemaphoreType.DMA
    tendency, signals = pl.pallas_call(
        functools.partial(kernel, sizes),
        out_shape=(
            jax.ShapeDtypeStruct((5, px, py, pz), F32),
            jax.ShapeDtypeStruct((1, own), F32),
        ),
        in_specs=[pl.BlockSpec(memory_space=pl.ANY)] * 7,
        out_specs=(pl.BlockSpec(memory_space=pltpu.VMEM), pl.BlockSpec(memory_space=pltpu.VMEM)),
        scratch_shapes=[
            pltpu.VMEM(density.shape, F32),
            pltpu.VMEM(velocity.shape, F32),
            pltpu.VMEM(pressure.shape, F32),
            pltpu.VMEM(blending.shape, F32),
            pltpu.VMEM(face_signal_weights.shape, BF16),
            pltpu.VMEM((1, slots), jnp.int32),
            pltpu.VMEM((1, slots), jnp.int32),
            pltpu.VMEM((5, px + 2, rows, lanes), F32),
            pltpu.VMEM((5, px, rows, lanes), F32),
            pltpu.VMEM((22, rows, lanes), F32),
            pltpu.VMEM((2, 5, rows, lanes), F32),
            pltpu.VMEM((2, 5, rows, lanes), F32),
            pltpu.VMEM((2, rows, 128), F32),
            pltpu.VMEM((2, rows, 128), F32),
            pltpu.VMEM((rows, pad), F32),
            pltpu.VMEM((groups - 1, rows, pad), F32),
            pltpu.VMEM((rows, shard_faces), F32),
            pltpu.VMEM((sizes[2] - 1, rows, shard_faces), F32),
            pltpu.VMEM((groups, 1, own), F32),
            pltpu.VMEM((groups - 1, 1, own), F32),
            dma((7,)),
            dma((6,)),
            dma((6,)),
            dma((groups - 1,)),
            dma((groups - 1,)),
            dma((sizes[2] - 1,)),
            dma((sizes[2] - 1,)),
            dma((groups - 1,)),
            dma((groups - 1,)),
        ],
        compiler_params=pltpu.CompilerParams(collective_id=0, has_side_effects=True),
    )(
        density, velocity, pressure, blending, face_signal_weights,
        surf_id.reshape(1, -1), surface_face_code.reshape(1, -1),
    )
    return tendency, signals.reshape(-1)


def solution(mesh):
    sizes = (mesh.shape["gx"], mesh.shape["gy"], mesh.shape["gz"])
    placed = (
        P("gx", "gy", "gz"),
        P(None, "gx", "gy", "gz"),
        P("gx", "gy", "gz"),
        P("gx", "gy", "gz"),
        P(None, ("gx", "gy"), "gz"),
        P(("gx", "gy", "gz")),
        P(("gx", "gy", "gz")),
    )
    return jax.shard_map(
        functools.partial(shards, sizes),
        mesh=mesh,
        in_specs=placed,
        out_specs=(P(None, "gx", "gy", "gz"), P(("gz", "gx", "gy"))),
        check_vma=False,
    )
```

```python
import functools
import math

import jax
import jax.numpy as jnp
import numpy as np
from jax import lax
from jax.experimental import pallas as pl
from jax.experimental.pallas import tpu as pltpu
from jax.sharding import PartitionSpec as P

GAMMA = 1.4
MESH = pl.DeviceIdType.MESH
F32 = jnp.float32
BF16 = jnp.bfloat16


def gauss_lobatto():
    inner_root = math.sqrt(3.0 / 7.0)
    points = np.array([-1.0, -inner_root, 0.0, inner_root, 1.0])
    quad_weights = np.array([0.1, 49.0 / 90.0, 32.0 / 45.0, 49.0 / 90.0, 0.1])
    barycentric = np.ones(5)
    for target in range(5):
        for source in range(5):
            if source != target:
                barycentric[target] = barycentric[target] / (points[target] - points[source])
    derivative = np.zeros((5, 5))
    for target in range(5):
        for source in range(5):
            if source != target:
                derivative[target, source] = (
                    barycentric[source] / barycentric[target] / (points[target] - points[source])
                )
        derivative[target, target] = -np.sum(derivative[target])
    return (derivative, quad_weights)


DERIV, QUAD = gauss_lobatto()
NODES = len(QUAD)


def up(value, step):
    return (value + step - 1) // step * step


def pick(index, table):
    out = jnp.zeros(index.shape, F32)
    for key, value in table.items():
        out = jnp.where(index == key, F32(value), out)
    return out


def with_energy(prim):
    rho, u, v, w, p = prim
    specific = p / rho * (1.0 / (GAMMA - 1.0)) + 0.5 * (u * u + v * v + w * w)
    return (rho, u, v, w, specific, p)


def pair_flux(a, b, d):
    r, s1, s2, s3, se, sp = (x + y for x, y in zip(a, b))
    speeds = (s1, s2, s3)
    m = r * speeds[d]
    parts = [m + m]
    for c in range(3):
        parts.append(m * speeds[c] + 4.0 * sp if c == d else m * speeds[c])
    parts.append(m * se + 2.0 * (sp * speeds[d]))
    return parts


def node_state(a, d):
    rho, u, v, w, specific, p = a
    speeds = (u, v, w)
    energy = rho * specific
    cons = [rho, rho * u, rho * v, rho * w, energy]
    normal = speeds[d]
    flux = [cons[1 + d]]
    for c in range(3):
        part = cons[1 + c] * normal
        flux.append(part + p if c == d else part)
    flux.append((energy + p) * normal)
    return flux, cons, jnp.abs(normal) + jnp.sqrt(GAMMA * (p / rho))


def rusanov2(left, right):
    (fl, ul, sl), (fr, ur, sr) = left, right
    fastest = jnp.maximum(sl, sr)
    return [a + b - fastest * (d - c) for a, b, c, d in zip(fl, fr, ul, ur)]


def kernel(
    sizes,
    den_h, vel_h, pre_h, ble_h, wei_h, id_h, code_h,
    tend_ref, sig_ref,
    den, vel, pre, ble, wei, ids, codes,
    prim, acc, coef, ystage, yghost, zstage, zghost,
    mine, faces_in, part, parts_in, stage, sums_in,
    in_sem, halo_send, halo_recv, face_send, face_recv, z_send, z_recv, rs_send, rs_recv,
):
    nx_dev, ny_dev, nz_dev = sizes
    groups = nx_dev * ny_dev
    px, py, pz = den_h.shape
    elems = ble_h.shape[-1]
    slots = id_h.shape[-1]
    lanes = prim.shape[-1]
    rows = prim.shape[-2]
    quantities, shard_faces, local_signals = wei_h.shape
    own = local_signals // groups

    gx, gy, gz = lax.axis_index("gx"), lax.axis_index("gy"), lax.axis_index("gz")
    group = gx * ny_dev + gy

    def in_group(step):
        other = lax.rem(group + step, groups)
        return (lax.div(other, ny_dev), lax.rem(other, ny_dev), gz)

    def in_column(step):
        return (gx, gy, lax.rem(gz + step, nz_dev))

    barrier = pltpu.get_barrier_semaphore()
    for step in range(1, groups):
        pl.semaphore_signal(barrier, inc=1, device_id=in_group(step), device_id_type=MESH)
    for step in range(1, nz_dev):
        pl.semaphore_signal(barrier, inc=1, device_id=in_column(step), device_id_type=MESH)

    loads = [
        pltpu.make_async_copy(src, dst, in_sem.at[n])
        for n, (src, dst) in enumerate(
            ((den_h, den), (vel_h, vel), (pre_h, pre), (ble_h, ble), (id_h, ids), (code_h, codes), (wei_h, wei))
        )
    ]
    for load in loads:
        load.start()

    row = lax.broadcasted_iota(jnp.int32, (rows, lanes), 0)
    lane = lax.broadcasted_iota(jnp.int32, (rows, lanes), 1)
    lane_node = lax.rem(lane, NODES)
    row_weight = pick(row, {i: QUAD[i] for i in range(NODES)})

    width = up(3 * elems, 128)
    z_at = lax.broadcasted_iota(jnp.int32, (lanes, width), 0)
    c_at = lax.broadcasted_iota(jnp.int32, (lanes, width), 1)
    element = lax.div(z_at, NODES)
    node = z_at - NODES * element
    reduce_z = jnp.where(element == c_at, pick(node, {i: QUAD[i] for i in range(NODES)}), F32(0))
    reduce_z = jnp.where((element + elems == c_at) & (node == 0), F32(-1), reduce_z)
    reduce_z = jnp.where((element + 2 * elems == c_at) & (node == NODES - 1), F32(1), reduce_z)
    reduce_z = jnp.where(z_at < pz, reduce_z, F32(0))

    prim[:, 0:px] = jnp.ones((5, px, rows, lanes), F32)
    for n in range(3):
        loads[n].wait()
    for x in range(px):
        prim[0, x, 0:py, 0:pz] = den[x]
        for c in range(3):
            prim[1 + c, x, 0:py, 0:pz] = vel[x, :, c, :]
        prim[4, x, 0:py, 0:pz] = pre[x]

    def mass_momentum(x, d):
        rho, u, v, w, p = (prim[f, x] for f in range(5))
        speeds = (u, v, w)
        m = rho * speeds[d]
        return [m] + [m * speeds[c] + p if c == d else m * speeds[c] for c in range(3)]

    def rows_of(values, sign):
        out = jnp.zeros((rows, lanes), F32)
        for q in range(quantities):
            out = jnp.where(row == q, sign * values[q], out)
        return out

    tables = []
    for x, sign in ((0, -1.0), (px - 1, 1.0)):
        sums = [jnp.sum(row_weight * f, axis=0, keepdims=True) for f in mass_momentum(x, 0)]
        tables.append(rows_of(sums, sign))
    along_y = [jnp.zeros((rows, lanes), F32)] * quantities
    along_z = [jnp.zeros((rows, lanes), F32)] * quantities
    for x in range(px):
        along_y = [a + F32(QUAD[x]) * f for a, f in zip(along_y, mass_momentum(x, 1))]
        along_z = [a + F32(QUAD[x]) * f for a, f in zip(along_z, mass_momentum(x, 2))]
    for y, sign in ((0, -1.0), (py - 1, 1.0)):
        tables.append(rows_of([a[y : y + 1] for a in along_y], sign))
    tables.append(rows_of([jnp.sum(row_weight * a, axis=0, keepdims=True) for a in along_z], 1.0))
    table = jnp.dot(
        jnp.concatenate(tables, axis=0), reduce_z,
        precision=lax.Precision.HIGHEST, preferred_element_type=F32,
    ).astype(BF16)

    for n in range(3, 6):
        loads[n].wait()
    pad = mine.shape[-1]
    code_row = jnp.concatenate([codes[...], jnp.full((1, pad - slots), -1, jnp.int32)], axis=1) if pad > slots else codes[...]
    id_row = jnp.concatenate([ids[...], jnp.full((1, pad - slots), -1, jnp.int32)], axis=1) if pad > slots else ids[...]
    r_at = lax.broadcasted_iota(jnp.int32, (width, pad), 0)
    chosen = []
    for f in range(4):
        hit = (code_row == r_at + f * elems) & (r_at < elems)
        chosen.append(jnp.where(hit, F32(1), F32(0)).astype(BF16))
    hit = (code_row == r_at + 3 * elems) & (r_at >= elems) & (r_at < 3 * elems)
    chosen.append(jnp.where(hit, F32(1), F32(0)).astype(BF16))
    face_values = jnp.dot(
        jnp.concatenate([table[rows * f : rows * f + rows] for f in range(5)], axis=1),
        jnp.concatenate(chosen, axis=0),
        preferred_element_type=F32,
    )
    slot_row = lax.broadcasted_iota(jnp.int32, (rows, pad), 0)
    mine[...] = jnp.where(slot_row == quantities, id_row.astype(F32), face_values)

    ystage[...] = jnp.ones(ystage.shape, F32)
    for x in range(px):
        for f in range(5):
            ystage[0, f, x : x + 1, :] = prim[f, x, 0:1, :]
            ystage[1, f, x : x + 1, :] = prim[f, x, py - 1 : py, :]
    zlane = lax.broadcasted_iota(jnp.int32, (rows, 128), 1)
    for side, at in ((0, 0), (1, pz - 1)):
        packed = jnp.ones((rows, 128), F32)
        for f in range(5):
            for x in range(px):
                packed = jnp.where(zlane == f * px + x, prim[f, x, :, at : at + 1], packed)
        zstage[side] = packed

    pl.semaphore_wait(barrier, groups - 1 + nz_dev - 1)

    def remote(src, dst, send, recv, device):
        return pltpu.make_async_remote_copy(
            src_ref=src, dst_ref=dst, send_sem=send, recv_sem=recv, device_id=device, device_id_type=MESH
        )

    face_copies = [
        remote(mine, faces_in.at[k - 1], face_send.at[k - 1], face_recv.at[k - 1], in_group(k))
        for k in range(1, groups)
    ]
    for copy in face_copies:
        copy.start()

    def beside(axis, step):
        at = [gx, gy, gz]
        at[axis] = lax.rem(at[axis] + sizes[axis] + step, sizes[axis])
        return tuple(at)

    halo_copies = [
        remote(prim.at[:, px - 1], prim.at[:, px + 1], halo_send.at[0], halo_recv.at[0], beside(0, 1)),
        remote(prim.at[:, 0], prim.at[:, px], halo_send.at[1], halo_recv.at[1], beside(0, -1)),
        remote(ystage.at[1], yghost.at[0], halo_send.at[2], halo_recv.at[2], beside(1, 1)),
        remote(ystage.at[0], yghost.at[1], halo_send.at[3], halo_recv.at[3], beside(1, -1)),
        remote(zstage.at[1], zghost.at[0], halo_send.at[4], halo_recv.at[4], beside(2, 1)),
        remote(zstage.at[0], zghost.at[1], halo_send.at[5], halo_recv.at[5], beside(2, -1)),
    ]
    for copy in halo_copies:
        copy.start()

    spread_e = lax.broadcasted_iota(jnp.int32, (elems, lanes), 0)
    spread_z = lax.broadcasted_iota(jnp.int32, (elems, lanes), 1)
    spread = jnp.where(lax.div(spread_z, NODES) == spread_e, F32(1), F32(0))
    alpha = jnp.dot(
        jnp.broadcast_to(ble[0], (rows, elems)), spread,
        precision=lax.Precision.HIGHEST, preferred_element_type=F32,
    )
    volume = jnp.where(lane < pz, (alpha - 1.0) * 0.25, F32(0))
    for d, at in ((0, row), (1, lane_node)):
        for k in range(1, NODES):
            base = 8 * d + 2 * (k - 1)
            coef[base] = volume * pick(at, {i: DERIV[i, i + k] for i in range(NODES - k)})
            coef[base + 1] = volume * pick(at, {i: DERIV[i + k, i] for i in range(NODES - k)})
        half = pick(at, {i: 0.5 / QUAD[i] for i in range(NODES)})
        coef[16 + 2 * d] = -half * jnp.where(at == NODES - 1, F32(1), alpha)
        coef[17 + 2 * d] = half * jnp.where(at == 0, F32(1), alpha)
    coef[20] = volume
    coef[21] = alpha

    def plane(x):
        return with_energy(tuple(prim[f, x] for f in range(5)))

    def inside(x, carry):
        here = plane(x)
        total = [acc[q, x] for q in range(5)]
        for d, axis, size in ((1, 0, rows), (2, 1, lanes)):
            for k in range(1, NODES):
                there = tuple(pltpu.roll(a, size - k, axis) for a in here)
                flux = pair_flux(here, there, d)
                base = 8 * (d - 1) + 2 * (k - 1)
                forward, back = coef[base], coef[base + 1]
                total = [t + forward * f + pltpu.roll(back * f, k, axis) for t, f in zip(total, flux)]
        for q in range(5):
            acc[q, x] = total[q]
        return carry

    planes = [plane(x) for x in range(px)]
    for x in range(px):
        total = [jnp.zeros((rows, lanes), F32)] * 5
        for other in range(px):
            if other != x:
                flux = pair_flux(planes[x], planes[other], 0)
                total = [t + F32(DERIV[x, other]) * f for t, f in zip(total, flux)]
        for q in range(5):
            acc[q, x] = coef[20] * total[q]
    lax.fori_loop(0, px, inside, 0, unroll=True)

    for copy in face_copies:
        copy.wait()
    wanted = lax.broadcasted_iota(jnp.int32, (shard_faces, pad), 0).astype(F32)
    start = (group * shard_faces).astype(F32)
    arrived = [mine[...]] + [faces_in[k] for k in range(groups - 1)]
    placing = [
        jnp.where(a[quantities : quantities + 1] - start == wanted, F32(1), F32(0)).astype(BF16) for a in arrived
    ]
    part[...] = lax.dot_general(
        jnp.concatenate([a.astype(BF16) for a in arrived], axis=1),
        jnp.concatenate(placing, axis=1),
        (((1,), (1,)), ((), ())),
        preferred_element_type=F32,
    )
    z_copies = [
        remote(part, parts_in.at[k - 1], z_send.at[k - 1], z_recv.at[k - 1], in_column(k))
        for k in range(1, nz_dev)
    ]
    for copy in z_copies:
        copy.start()

    for copy in halo_copies:
        copy.wait()
    low, high = zghost[0], zghost[1]
    for f in range(5):
        for x in range(px):
            prim[f, x, py : py + 1, :] = yghost[1, f, x : x + 1, :]
            prim[f, x, rows - 1 : rows, :] = yghost[0, f, x : x + 1, :]
            at = f * px + x
            first = pz // 128 * 128
            block = prim[f, x, :, first : first + 128]
            block = jnp.where(zlane == pz - first, high[:, at : at + 1], block)
            if first + 128 == lanes:
                block = jnp.where(zlane == 127, low[:, at : at + 1], block)
            else:
                last = prim[f, x, :, lanes - 128 : lanes]
                prim[f, x, :, lanes - 128 : lanes] = jnp.where(zlane == 127, low[:, at : at + 1], last)
            prim[f, x, :, first : first + 128] = block

    def between(x, carry):
        here = plane(x)
        total = [acc[q, x] for q in range(5)]
        for d, axis, size in ((1, 0, rows), (2, 1, lanes)):
            state = node_state(here, d)
            after = (
                [pltpu.roll(a, size - 1, axis) for a in state[0]],
                [pltpu.roll(a, size - 1, axis) for a in state[1]],
                pltpu.roll(state[2], size - 1, axis),
            )
            upper, lower = coef[14 + 2 * d], coef[15 + 2 * d]
            edge = rusanov2(state, after)
            total = [t + upper * e + lower * pltpu.roll(e, 1, axis) for t, e in zip(total, edge)]
        for q in range(5):
            acc[q, x] = total[q]
        return carry

    lax.fori_loop(0, px, between, 0, unroll=True)

    before = node_state(plane(px + 1), 0)
    current = node_state(plane(0), 0)
    below = rusanov2(before, current)
    for x in range(px):
        following = node_state(plane(x + 1), 0)
        above = rusanov2(current, following)
        half = F32(0.5 / QUAD[x])
        for q in range(5):
            out = acc[q, x]
            mix = coef[21] * half
            out = out - (half if x == px - 1 else mix) * above[q]
            out = out + (half if x == 0 else mix) * below[q]
            tend_ref[q, x] = out[0:py, 0:pz]
        current, below = following, above

    for copy in z_copies:
        copy.wait()
    loads[6].wait()
    data = part[...]
    for k in range(nz_dev - 1):
        data = data + parts_in[k]
    data = data.astype(BF16)
    data_row = lax.broadcasted_iota(jnp.int32, data.shape, 0)
    result = jnp.zeros((rows, local_signals), F32)
    for q in range(quantities):
        result = result + jnp.dot(
            jnp.where(data_row == q, data, jnp.zeros((), BF16)), wei[q], preferred_element_type=F32
        )
    result = jnp.sum(result, axis=0, keepdims=True)
    for t in range(groups):
        stage[t] = result[:, t * own : (t + 1) * own]
    rs_copies = []
    for k in range(1, groups):
        other = lax.rem(group + k, groups)
        rs_copies.append(
            remote(stage.at[other], sums_in.at[k - 1], rs_send.at[k - 1], rs_recv.at[k - 1], in_group(k))
        )
    for copy in rs_copies:
        copy.start()
    for copy in rs_copies:
        copy.wait()
    total = stage[group]
    for k in range(groups - 1):
        total = total + sums_in[k]
    sig_ref[...] = total


def write_out(tend_ref, sig_ref, tend_h, sig_h, sem):
    copies = (
        pltpu.make_async_copy(tend_ref, tend_h, sem.at[0]),
        pltpu.make_async_copy(sig_ref, sig_h, sem.at[1]),
    )
    for copy in copies:
        copy.start()
    for copy in copies:
        copy.wait()


def shards(sizes, density, velocity, pressure, blending, face_signal_weights, surf_id, surface_face_code):
    groups = sizes[0] * sizes[1]
    px, py, pz = density.shape
    assert blending.shape[:2] == (1, 1) and px == NODES and py == NODES
    rows, lanes = up(py + 2, 8), up(pz + 2, 128)
    slots = surf_id.shape[0]
    pad = up(slots, 128)
    quantities, shard_faces, local_signals = face_signal_weights.shape
    own = local_signals // groups
    dma = pltpu.SemaphoreType.DMA
    tendency, signals = pl.pallas_call(
        functools.partial(kernel, sizes),
        out_shape=(pltpu.VMEM((5, px, py, pz), F32), pltpu.VMEM((1, own), F32)),
        in_specs=[pl.BlockSpec(memory_space=pl.ANY)] * 7,
        out_specs=(pl.BlockSpec(memory_space=pltpu.VMEM), pl.BlockSpec(memory_space=pltpu.VMEM)),
        scratch_shapes=[
            pltpu.VMEM(density.shape, F32),
            pltpu.VMEM((px, py, 3, pz), F32),
            pltpu.VMEM(pressure.shape, F32),
            pltpu.VMEM(blending.shape, F32),
            pltpu.VMEM(face_signal_weights.shape, BF16),
            pltpu.VMEM((1, slots), jnp.int32),
            pltpu.VMEM((1, slots), jnp.int32),
            pltpu.VMEM((5, px + 2, rows, lanes), F32),
            pltpu.VMEM((5, px, rows, lanes), F32),
            pltpu.VMEM((22, rows, lanes), F32),
            pltpu.VMEM((2, 5, rows, lanes), F32),
            pltpu.VMEM((2, 5, rows, lanes), F32),
            pltpu.VMEM((2, rows, 128), F32),
            pltpu.VMEM((2, rows, 128), F32),
            pltpu.VMEM((rows, pad), F32),
            pltpu.VMEM((groups - 1, rows, pad), F32),
            pltpu.VMEM((rows, shard_faces), F32),
            pltpu.VMEM((sizes[2] - 1, rows, shard_faces), F32),
            pltpu.VMEM((groups, 1, own), F32),
            pltpu.VMEM((groups - 1, 1, own), F32),
            dma((7,)),
            dma((6,)),
            dma((6,)),
            dma((groups - 1,)),
            dma((groups - 1,)),
            dma((sizes[2] - 1,)),
            dma((sizes[2] - 1,)),
            dma((groups - 1,)),
            dma((groups - 1,)),
        ],
        compiler_params=pltpu.CompilerParams(collective_id=0, has_side_effects=True),
    )(
        density, jnp.transpose(velocity, (1, 2, 0, 3)), pressure, blending, face_signal_weights,
        surf_id.reshape(1, -1), surface_face_code.reshape(1, -1),
    )
    tendency = pltpu.with_memory_space_constraint(tendency, pltpu.VMEM)
    signals = pltpu.with_memory_space_constraint(signals, pltpu.VMEM)
    tendency, signals = pl.pallas_call(
        write_out,
        out_shape=(
            jax.ShapeDtypeStruct((5, px, py, pz), F32),
            jax.ShapeDtypeStruct((1, own), F32),
        ),
        in_specs=[pl.BlockSpec(memory_space=pltpu.VMEM)] * 2,
        out_specs=(pl.BlockSpec(memory_space=pl.ANY), pl.BlockSpec(memory_space=pl.ANY)),
        scratch_shapes=[dma((2,))],
    )(tendency, signals)
    return tendency, signals.reshape(-1)


def solution(mesh):
    sizes = (mesh.shape["gx"], mesh.shape["gy"], mesh.shape["gz"])
    placed = (
        P("gx", "gy", "gz"),
        P(None, "gx", "gy", "gz"),
        P("gx", "gy", "gz"),
        P("gx", "gy", "gz"),
        P(None, ("gx", "gy"), "gz"),
        P(("gx", "gy", "gz")),
        P(("gx", "gy", "gz")),
    )
    return jax.shard_map(
        functools.partial(shards, sizes),
        mesh=mesh,
        in_specs=placed,
        out_specs=(P(None, "gx", "gy", "gz"), P(("gz", "gx", "gy"))),
        check_vma=False,
    )
```

```python
import functools
import math

import jax
import jax.numpy as jnp
import numpy as np
from jax import lax
from jax.experimental import pallas as pl
from jax.experimental.pallas import tpu as pltpu
from jax.sharding import PartitionSpec as P

GAMMA = 1.4
MESH = pl.DeviceIdType.MESH
F32 = jnp.float32
BF16 = jnp.bfloat16


def gauss_lobatto():
    inner_root = math.sqrt(3.0 / 7.0)
    points = np.array([-1.0, -inner_root, 0.0, inner_root, 1.0])
    quad_weights = np.array([0.1, 49.0 / 90.0, 32.0 / 45.0, 49.0 / 90.0, 0.1])
    barycentric = np.ones(5)
    for target in range(5):
        for source in range(5):
            if source != target:
                barycentric[target] = barycentric[target] / (points[target] - points[source])
    derivative = np.zeros((5, 5))
    for target in range(5):
        for source in range(5):
            if source != target:
                derivative[target, source] = (
                    barycentric[source] / barycentric[target] / (points[target] - points[source])
                )
        derivative[target, target] = -np.sum(derivative[target])
    return (derivative, quad_weights)


DERIV, QUAD = gauss_lobatto()
NODES = len(QUAD)


def up(value, step):
    return (value + step - 1) // step * step


def pick(index, table):
    out = jnp.zeros(index.shape, F32)
    for key, value in table.items():
        out = jnp.where(index == key, F32(value), out)
    return out


def with_energy(prim):
    rho, u, v, w, p = prim
    specific = p / rho * (1.0 / (GAMMA - 1.0)) + 0.5 * (u * u + v * v + w * w)
    return (rho, u, v, w, specific, p)


def pair_flux(a, b, d):
    r, s1, s2, s3, se, sp = (x + y for x, y in zip(a, b))
    speeds = (s1, s2, s3)
    m = r * speeds[d]
    parts = [m + m]
    for c in range(3):
        parts.append(m * speeds[c] + 4.0 * sp if c == d else m * speeds[c])
    parts.append(m * se + 2.0 * (sp * speeds[d]))
    return parts


def node_state(a, d):
    rho, u, v, w, specific, p = a
    speeds = (u, v, w)
    energy = rho * specific
    cons = [rho, rho * u, rho * v, rho * w, energy]
    normal = speeds[d]
    flux = [cons[1 + d]]
    for c in range(3):
        part = cons[1 + c] * normal
        flux.append(part + p if c == d else part)
    flux.append((energy + p) * normal)
    return flux, cons, jnp.abs(normal) + jnp.sqrt(GAMMA * (p / rho))


def rusanov2(left, right):
    (fl, ul, sl), (fr, ur, sr) = left, right
    fastest = jnp.maximum(sl, sr)
    return [a + b - fastest * (d - c) for a, b, c, d in zip(fl, fr, ul, ur)]


def kernel(
    sizes,
    den_h, vel_h, pre_h, ble_h, wei_h, id_h, code_h,
    tend_ref, sig_ref,
    den, vel, pre, ble, wei, ids, codes,
    prim, acc, coef, ystage, yghost, zstage, zghost,
    mine, faces_in, part, parts_in, stage, sums_in,
    in_sem, halo_send, halo_recv, face_send, face_recv, z_send, z_recv, rs_send, rs_recv,
):
    nx_dev, ny_dev, nz_dev = sizes
    groups = nx_dev * ny_dev
    px, py, pz = den_h.shape
    elems = ble_h.shape[-1]
    slots = id_h.shape[-1]
    lanes = prim.shape[-1]
    rows = prim.shape[-2]
    quantities, shard_faces, local_signals = wei_h.shape
    own = local_signals // groups

    gx, gy, gz = lax.axis_index("gx"), lax.axis_index("gy"), lax.axis_index("gz")
    group = gx * ny_dev + gy

    def in_group(step):
        other = lax.rem(group + step, groups)
        return (lax.div(other, ny_dev), lax.rem(other, ny_dev), gz)

    def in_column(step):
        return (gx, gy, lax.rem(gz + step, nz_dev))

    barrier = pltpu.get_barrier_semaphore()
    for step in range(1, groups):
        pl.semaphore_signal(barrier, inc=1, device_id=in_group(step), device_id_type=MESH)
    for step in range(1, nz_dev):
        pl.semaphore_signal(barrier, inc=1, device_id=in_column(step), device_id_type=MESH)

    loads = [
        pltpu.make_async_copy(src, dst, in_sem.at[n])
        for n, (src, dst) in enumerate(
            ((den_h, den), (vel_h, vel), (pre_h, pre), (ble_h, ble), (id_h, ids), (code_h, codes), (wei_h, wei))
        )
    ]
    for load in loads:
        load.start()

    row = lax.broadcasted_iota(jnp.int32, (rows, lanes), 0)
    lane = lax.broadcasted_iota(jnp.int32, (rows, lanes), 1)
    lane_node = lax.rem(lane, NODES)
    row_weight = pick(row, {i: QUAD[i] for i in range(NODES)})

    width = up(3 * elems, 128)
    z_at = lax.broadcasted_iota(jnp.int32, (lanes, width), 0)
    c_at = lax.broadcasted_iota(jnp.int32, (lanes, width), 1)
    element = lax.div(z_at, NODES)
    node = z_at - NODES * element
    reduce_z = jnp.where(element == c_at, pick(node, {i: QUAD[i] for i in range(NODES)}), F32(0))
    reduce_z = jnp.where((element + elems == c_at) & (node == 0), F32(-1), reduce_z)
    reduce_z = jnp.where((element + 2 * elems == c_at) & (node == NODES - 1), F32(1), reduce_z)
    reduce_z = jnp.where(z_at < pz, reduce_z, F32(0))

    prim[:, 0:px] = jnp.ones((5, px, rows, lanes), F32)
    for n in range(3):
        loads[n].wait()
    for x in range(px):
        prim[0, x, 0:py, 0:pz] = den[x]
        for c in range(3):
            prim[1 + c, x, 0:py, 0:pz] = vel[x, :, c, :]
        prim[4, x, 0:py, 0:pz] = pre[x]

    def mass_momentum(x, d):
        rho, u, v, w, p = (prim[f, x] for f in range(5))
        speeds = (u, v, w)
        m = rho * speeds[d]
        return [m] + [m * speeds[c] + p if c == d else m * speeds[c] for c in range(3)]

    def rows_of(values, sign):
        out = jnp.zeros((rows, lanes), F32)
        for q in range(quantities):
            out = jnp.where(row == q, sign * values[q], out)
        return out

    tables = []
    for x, sign in ((0, -1.0), (px - 1, 1.0)):
        sums = [jnp.sum(row_weight * f, axis=0, keepdims=True) for f in mass_momentum(x, 0)]
        tables.append(rows_of(sums, sign))
    along_y = [jnp.zeros((rows, lanes), F32)] * quantities
    along_z = [jnp.zeros((rows, lanes), F32)] * quantities
    for x in range(px):
        along_y = [a + F32(QUAD[x]) * f for a, f in zip(along_y, mass_momentum(x, 1))]
        along_z = [a + F32(QUAD[x]) * f for a, f in zip(along_z, mass_momentum(x, 2))]
    for y, sign in ((0, -1.0), (py - 1, 1.0)):
        tables.append(rows_of([a[y : y + 1] for a in along_y], sign))
    tables.append(rows_of([jnp.sum(row_weight * a, axis=0, keepdims=True) for a in along_z], 1.0))
    table = jnp.dot(
        jnp.concatenate(tables, axis=0), reduce_z,
        precision=lax.Precision.HIGHEST, preferred_element_type=F32,
    ).astype(BF16)

    for n in range(3, 6):
        loads[n].wait()
    pad = up(slots, 128)
    code_row = jnp.concatenate([codes[...], jnp.full((1, pad - slots), -1, jnp.int32)], axis=1) if pad > slots else codes[...]
    id_row = jnp.concatenate([ids[...], jnp.full((1, pad - slots), -1, jnp.int32)], axis=1) if pad > slots else ids[...]
    r_at = lax.broadcasted_iota(jnp.int32, (width, pad), 0)
    chosen = []
    for f in range(4):
        hit = (code_row == r_at + f * elems) & (r_at < elems)
        chosen.append(jnp.where(hit, F32(1), F32(0)).astype(BF16))
    hit = (code_row == r_at + 3 * elems) & (r_at >= elems) & (r_at < 3 * elems)
    chosen.append(jnp.where(hit, F32(1), F32(0)).astype(BF16))
    face_values = jnp.dot(
        jnp.concatenate([table[rows * f : rows * f + rows] for f in range(5)], axis=1),
        jnp.concatenate(chosen, axis=0),
        preferred_element_type=F32,
    )
    face_values = face_values.astype(BF16)
    wanted = lax.broadcasted_iota(jnp.int32, (shard_faces, pad), 0)
    for t in range(groups):
        placing = jnp.where(id_row == wanted + t * shard_faces, F32(1), F32(0)).astype(BF16)
        mine[t] = lax.dot_general(
            face_values, placing, (((1,), (1,)), ((), ())), preferred_element_type=F32
        ).astype(BF16)

    ystage[...] = jnp.ones(ystage.shape, F32)
    for x in range(px):
        for f in range(5):
            ystage[0, f, x : x + 1, :] = prim[f, x, 0:1, :]
            ystage[1, f, x : x + 1, :] = prim[f, x, py - 1 : py, :]
    zlane = lax.broadcasted_iota(jnp.int32, (rows, 128), 1)
    for side, at in ((0, 0), (1, pz - 1)):
        packed = jnp.ones((rows, 128), F32)
        for f in range(5):
            for x in range(px):
                packed = jnp.where(zlane == f * px + x, prim[f, x, :, at : at + 1], packed)
        zstage[side] = packed

    pl.semaphore_wait(barrier, groups - 1 + nz_dev - 1)

    def remote(src, dst, send, recv, device):
        return pltpu.make_async_remote_copy(
            src_ref=src, dst_ref=dst, send_sem=send, recv_sem=recv, device_id=device, device_id_type=MESH
        )

    face_copies = [
        remote(
            mine.at[lax.rem(group + k, groups)], faces_in.at[k - 1],
            face_send.at[k - 1], face_recv.at[k - 1], in_group(k),
        )
        for k in range(1, groups)
    ]
    for copy in face_copies:
        copy.start()

    def beside(axis, step):
        at = [gx, gy, gz]
        at[axis] = lax.rem(at[axis] + sizes[axis] + step, sizes[axis])
        return tuple(at)

    halo_copies = [
        remote(prim.at[:, px - 1], prim.at[:, px + 1], halo_send.at[0], halo_recv.at[0], beside(0, 1)),
        remote(prim.at[:, 0], prim.at[:, px], halo_send.at[1], halo_recv.at[1], beside(0, -1)),
        remote(ystage.at[1], yghost.at[0], halo_send.at[2], halo_recv.at[2], beside(1, 1)),
        remote(ystage.at[0], yghost.at[1], halo_send.at[3], halo_recv.at[3], beside(1, -1)),
        remote(zstage.at[1], zghost.at[0], halo_send.at[4], halo_recv.at[4], beside(2, 1)),
        remote(zstage.at[0], zghost.at[1], halo_send.at[5], halo_recv.at[5], beside(2, -1)),
    ]
    for copy in halo_copies:
        copy.start()

    spread_e = lax.broadcasted_iota(jnp.int32, (elems, lanes), 0)
    spread_z = lax.broadcasted_iota(jnp.int32, (elems, lanes), 1)
    spread = jnp.where(lax.div(spread_z, NODES) == spread_e, F32(1), F32(0))
    alpha = jnp.dot(
        jnp.broadcast_to(ble[0], (rows, elems)), spread,
        precision=lax.Precision.HIGHEST, preferred_element_type=F32,
    )
    volume = jnp.where(lane < pz, (alpha - 1.0) * 0.25, F32(0))
    for d, at in ((0, row), (1, lane_node)):
        for k in range(1, NODES):
            base = 8 * d + 2 * (k - 1)
            coef[base] = volume * pick(at, {i: DERIV[i, i + k] for i in range(NODES - k)})
            coef[base + 1] = volume * pick(at, {i: DERIV[i + k, i] for i in range(NODES - k)})
        half = pick(at, {i: 0.5 / QUAD[i] for i in range(NODES)})
        coef[16 + 2 * d] = -half * jnp.where(at == NODES - 1, F32(1), alpha)
        coef[17 + 2 * d] = half * jnp.where(at == 0, F32(1), alpha)
    coef[20] = volume
    coef[21] = alpha

    def plane(x):
        return with_energy(tuple(prim[f, x] for f in range(5)))

    def inside(x, carry):
        here = plane(x)
        total = [acc[q, x] for q in range(5)]
        for d, axis, size in ((1, 0, rows), (2, 1, lanes)):
            for k in range(1, NODES):
                there = tuple(pltpu.roll(a, size - k, axis) for a in here)
                flux = pair_flux(here, there, d)
                base = 8 * (d - 1) + 2 * (k - 1)
                forward, back = coef[base], coef[base + 1]
                total = [t + forward * f + pltpu.roll(back * f, k, axis) for t, f in zip(total, flux)]
        for q in range(5):
            acc[q, x] = total[q]
        return carry

    planes = [plane(x) for x in range(px)]
    for x in range(px):
        total = [jnp.zeros((rows, lanes), F32)] * 5
        for other in range(px):
            if other != x:
                flux = pair_flux(planes[x], planes[other], 0)
                total = [t + F32(DERIV[x, other]) * f for t, f in zip(total, flux)]
        for q in range(5):
            acc[q, x] = coef[20] * total[q]
    lax.fori_loop(0, px, inside, 0, unroll=True)

    for copy in face_copies:
        copy.wait()
    summed = mine[group].astype(F32)
    for k in range(groups - 1):
        summed = summed + faces_in[k].astype(F32)
    part[...] = summed.astype(BF16)
    z_copies = [
        remote(part, parts_in.at[k - 1], z_send.at[k - 1], z_recv.at[k - 1], in_column(k))
        for k in range(1, nz_dev)
    ]
    for copy in z_copies:
        copy.start()

    for copy in halo_copies:
        copy.wait()
    low, high = zghost[0], zghost[1]
    for f in range(5):
        for x in range(px):
            prim[f, x, py : py + 1, :] = yghost[1, f, x : x + 1, :]
            prim[f, x, rows - 1 : rows, :] = yghost[0, f, x : x + 1, :]
            at = f * px + x
            first = pz // 128 * 128
            block = prim[f, x, :, first : first + 128]
            block = jnp.where(zlane == pz - first, high[:, at : at + 1], block)
            if first + 128 == lanes:
                block = jnp.where(zlane == 127, low[:, at : at + 1], block)
            else:
                last = prim[f, x, :, lanes - 128 : lanes]
                prim[f, x, :, lanes - 128 : lanes] = jnp.where(zlane == 127, low[:, at : at + 1], last)
            prim[f, x, :, first : first + 128] = block

    def between(x, carry):
        here = plane(x)
        total = [acc[q, x] for q in range(5)]
        for d, axis, size in ((1, 0, rows), (2, 1, lanes)):
            state = node_state(here, d)
            after = (
                [pltpu.roll(a, size - 1, axis) for a in state[0]],
                [pltpu.roll(a, size - 1, axis) for a in state[1]],
                pltpu.roll(state[2], size - 1, axis),
            )
            upper, lower = coef[14 + 2 * d], coef[15 + 2 * d]
            edge = rusanov2(state, after)
            total = [t + upper * e + lower * pltpu.roll(e, 1, axis) for t, e in zip(total, edge)]
        for q in range(5):
            acc[q, x] = total[q]
        return carry

    lax.fori_loop(0, px, between, 0, unroll=True)

    for copy in z_copies:
        copy.wait()
    loads[6].wait()
    data = part[...].astype(F32)
    for k in range(nz_dev - 1):
        data = data + parts_in[k].astype(F32)
    data = data.astype(BF16)
    data_row = lax.broadcasted_iota(jnp.int32, data.shape, 0)
    result = jnp.zeros((rows, local_signals), F32)
    for q in range(quantities):
        result = result + jnp.dot(
            jnp.where(data_row == q, data, jnp.zeros((), BF16)), wei[q], preferred_element_type=F32
        )
    result = jnp.sum(result, axis=0, keepdims=True)
    for t in range(groups):
        stage[t] = result[:, t * own : (t + 1) * own]
    rs_copies = []
    for k in range(1, groups):
        other = lax.rem(group + k, groups)
        rs_copies.append(
            remote(stage.at[other], sums_in.at[k - 1], rs_send.at[k - 1], rs_recv.at[k - 1], in_group(k))
        )
    for copy in rs_copies:
        copy.start()
    before = node_state(plane(px + 1), 0)
    current = node_state(plane(0), 0)
    below = rusanov2(before, current)
    for x in range(px):
        following = node_state(plane(x + 1), 0)
        above = rusanov2(current, following)
        half = F32(0.5 / QUAD[x])
        for q in range(5):
            out = acc[q, x]
            mix = coef[21] * half
            out = out - (half if x == px - 1 else mix) * above[q]
            out = out + (half if x == 0 else mix) * below[q]
            tend_ref[q, x] = out[0:py, 0:pz]
        current, below = following, above

    for copy in rs_copies:
        copy.wait()
    total = stage[group]
    for k in range(groups - 1):
        total = total + sums_in[k]
    sig_ref[...] = total


def write_out(tend_ref, sig_ref, tend_h, sig_h, sem):
    copies = (
        pltpu.make_async_copy(tend_ref, tend_h, sem.at[0]),
        pltpu.make_async_copy(sig_ref, sig_h, sem.at[1]),
    )
    for copy in copies:
        copy.start()
    for copy in copies:
        copy.wait()


def shards(sizes, density, velocity, pressure, blending, face_signal_weights, surf_id, surface_face_code):
    groups = sizes[0] * sizes[1]
    px, py, pz = density.shape
    assert blending.shape[:2] == (1, 1) and px == NODES and py == NODES
    rows, lanes = up(py + 2, 8), up(pz + 2, 128)
    slots = surf_id.shape[0]
    quantities, shard_faces, local_signals = face_signal_weights.shape
    own = local_signals // groups
    dma = pltpu.SemaphoreType.DMA
    tendency, signals = pl.pallas_call(
        functools.partial(kernel, sizes),
        out_shape=(pltpu.VMEM((5, px, py, pz), F32), pltpu.VMEM((1, own), F32)),
        in_specs=[pl.BlockSpec(memory_space=pl.ANY)] * 7,
        out_specs=(pl.BlockSpec(memory_space=pltpu.VMEM), pl.BlockSpec(memory_space=pltpu.VMEM)),
        scratch_shapes=[
            pltpu.VMEM(density.shape, F32),
            pltpu.VMEM((px, py, 3, pz), F32),
            pltpu.VMEM(pressure.shape, F32),
            pltpu.VMEM(blending.shape, F32),
            pltpu.VMEM(face_signal_weights.shape, BF16),
            pltpu.VMEM((1, slots), jnp.int32),
            pltpu.VMEM((1, slots), jnp.int32),
            pltpu.VMEM((5, px + 2, rows, lanes), F32),
            pltpu.VMEM((5, px, rows, lanes), F32),
            pltpu.VMEM((22, rows, lanes), F32),
            pltpu.VMEM((2, 5, rows, lanes), F32),
            pltpu.VMEM((2, 5, rows, lanes), F32),
            pltpu.VMEM((2, rows, 128), F32),
            pltpu.VMEM((2, rows, 128), F32),
            pltpu.VMEM((groups, rows, shard_faces), BF16),
            pltpu.VMEM((groups - 1, rows, shard_faces), BF16),
            pltpu.VMEM((rows, shard_faces), BF16),
            pltpu.VMEM((sizes[2] - 1, rows, shard_faces), BF16),
            pltpu.VMEM((groups, 1, own), F32),
            pltpu.VMEM((groups - 1, 1, own), F32),
            dma((7,)),
            dma((6,)),
            dma((6,)),
            dma((groups - 1,)),
            dma((groups - 1,)),
            dma((sizes[2] - 1,)),
            dma((sizes[2] - 1,)),
            dma((groups - 1,)),
            dma((groups - 1,)),
        ],
        compiler_params=pltpu.CompilerParams(collective_id=0, has_side_effects=True),
    )(
        density, jnp.transpose(velocity, (1, 2, 0, 3)), pressure, blending, face_signal_weights,
        surf_id.reshape(1, -1), surface_face_code.reshape(1, -1),
    )
    tendency = pltpu.with_memory_space_constraint(tendency, pltpu.VMEM)
    signals = pltpu.with_memory_space_constraint(signals, pltpu.VMEM)
    tendency, signals = pl.pallas_call(
        write_out,
        out_shape=(
            jax.ShapeDtypeStruct((5, px, py, pz), F32),
            jax.ShapeDtypeStruct((1, own), F32),
        ),
        in_specs=[pl.BlockSpec(memory_space=pltpu.VMEM)] * 2,
        out_specs=(pl.BlockSpec(memory_space=pl.ANY), pl.BlockSpec(memory_space=pl.ANY)),
        scratch_shapes=[dma((2,))],
    )(tendency, signals)
    return tendency, signals.reshape(-1)


def solution(mesh):
    sizes = (mesh.shape["gx"], mesh.shape["gy"], mesh.shape["gz"])
    placed = (
        P("gx", "gy", "gz"),
        P(None, "gx", "gy", "gz"),
        P("gx", "gy", "gz"),
        P("gx", "gy", "gz"),
        P(None, ("gx", "gy"), "gz"),
        P(("gx", "gy", "gz")),
        P(("gx", "gy", "gz")),
    )
    return jax.shard_map(
        functools.partial(shards, sizes),
        mesh=mesh,
        in_specs=placed,
        out_specs=(P(None, "gx", "gy", "gz"), P(("gz", "gx", "gy"))),
        check_vma=False,
    )
```
